16 devices in a mesh: data: 2 (over y, z), sp: 8 (over x, core).
Axes of the slice: x: 4, y: 2, z: 1, core: 2. Of those that a mesh axis runs over, the one named last changes fastest.
The devices are a block of a 4x4x8 slice.
Arguments:
- latent: bfloat16 [2, 128, 512, 1152], P('data', 'sp'), parts along dimension 0
- ln_gain: bfloat16 [4, 1152], replicated
- ln_bias: bfloat16 [4, 1152], replicated
- w_qkv: bfloat16 [2, 1152, 3, 16, 72], replicated
- w_out: bfloat16 [2, 16, 72, 1152], replicated
- w_up: bfloat16 [2, 1152, 4608], replicated
- w_down: bfloat16 [2, 4608, 1152], replicated
Outputs:
- output: bfloat16 [2, 128, 512, 1152], P('data', 'sp'), parts along dimension 0
There are 2 independent parts. The reference program is written for one: setup_inputs(seed, part) draws one part's arguments, and reference() takes and returns one part's arrays. A program takes and returns all parts, laid end to end along the dimension named above; an argument that names none is the same for every part.
All inputs are finite; a program needn't handle non-finite values.
Results may differ from the reference program's by a relative error of at most 0.012557.
Values are sent between devices in bfloat16 or wider.
A program may use at most 768 MiB of HBM per device.

```python
import jax
import jax.numpy as jnp
from jax import lax
from functools import partial

FRAMES = 128
PATCHES = 512
WIDTH = 1152
NUM_HEADS = 16
HEAD_DIM = WIDTH // NUM_HEADS
LN_EPS = 1e-6


def setup_inputs(seed: int = 0, part: int = 0) -> dict:
    part_key = jax.random.fold_in(jax.random.key(seed), part)
    noise_key, frame_key, patch_key = jax.random.split(part_key, 3)
    noise = jax.random.normal(noise_key, (1, FRAMES, PATCHES, WIDTH), jnp.float32)
    frame_sig = jax.random.normal(frame_key, (1, FRAMES, 1, WIDTH), jnp.float32)
    patch_sig = jax.random.normal(patch_key, (1, 1, PATCHES, WIDTH), jnp.float32)
    latent = 0.6 * noise + frame_sig + 0.8 * patch_sig
    weight_keys = jax.random.split(jax.random.key(seed + 1), 6)
    qk_boost = jnp.array([1.3, 1.3, 1.0], jnp.float32).reshape(1, 1, 3, 1, 1)
    ln_gain = 1.0 + 0.4 * jax.random.normal(weight_keys[0], (4, WIDTH), jnp.float32)
    ln_bias = 0.5 * jax.random.normal(weight_keys[1], (4, WIDTH), jnp.float32)
    w_qkv = jax.random.normal(weight_keys[2], (2, WIDTH, 3, NUM_HEADS, HEAD_DIM), jnp.float32) * qk_boost * WIDTH ** -0.5
    w_out = jax.random.normal(weight_keys[3], (2, NUM_HEADS, HEAD_DIM, WIDTH), jnp.float32) * WIDTH ** -0.5
    w_up = jax.random.normal(weight_keys[4], (2, WIDTH, 4 * WIDTH), jnp.float32) * WIDTH ** -0.5
    w_down = jax.random.normal(weight_keys[5], (2, 4 * WIDTH, WIDTH), jnp.float32) * (4 * WIDTH) ** -0.5
    return {
        'latent': latent.astype(jnp.bfloat16),
        'ln_gain': ln_gain.astype(jnp.bfloat16),
        'ln_bias': ln_bias.astype(jnp.bfloat16),
        'w_qkv': w_qkv.astype(jnp.bfloat16),
        'w_out': w_out.astype(jnp.bfloat16),
        'w_up': w_up.astype(jnp.bfloat16),
        'w_down': w_down.astype(jnp.bfloat16),
    }


def layer_norm(tokens, gain_vec, shift_vec):
    as_float = tokens.astype(jnp.float32)
    mean_val = jnp.mean(as_float, axis=-1, keepdims=True)
    centered = as_float - mean_val
    variance = jnp.mean(centered * centered, axis=-1, keepdims=True)
    normed = centered * lax.rsqrt(variance + LN_EPS) * gain_vec.astype(jnp.float32) + shift_vec.astype(jnp.float32)
    return normed.astype(jnp.bfloat16)


def seq_block(sequence, layer_idx, ln_gain, ln_bias, w_qkv, w_out, w_up, w_down):
    length = sequence.shape[0]
    normed = layer_norm(sequence, ln_gain[2 * layer_idx], ln_bias[2 * layer_idx])
    qkv_all = jnp.dot(normed, w_qkv[layer_idx].reshape(WIDTH, 3 * WIDTH), preferred_element_type=jnp.float32).astype(jnp.bfloat16)
    qkv_all = qkv_all.reshape(length, 3, NUM_HEADS, HEAD_DIM).astype(jnp.float32)
    scores = jnp.einsum('qhk,phk->hqp', qkv_all[:, 0], qkv_all[:, 1]) * HEAD_DIM ** -0.5
    attn_probs = jax.nn.softmax(scores, axis=-1).astype(jnp.bfloat16)
    attended = jnp.einsum('hqp,phk->qhk', attn_probs.astype(jnp.float32), qkv_all[:, 2]).astype(jnp.bfloat16)
    projected = jnp.dot(attended.reshape(length, WIDTH), w_out[layer_idx].reshape(WIDTH, WIDTH), preferred_element_type=jnp.float32)
    residual = (sequence.astype(jnp.float32) + projected).astype(jnp.bfloat16)
    normed_mlp = layer_norm(residual, ln_gain[2 * layer_idx + 1], ln_bias[2 * layer_idx + 1])
    hidden = jax.nn.gelu(jnp.dot(normed_mlp, w_up[layer_idx], preferred_element_type=jnp.float32), approximate=True).astype(jnp.bfloat16)
    result = residual.astype(jnp.float32) + jnp.dot(hidden, w_down[layer_idx], preferred_element_type=jnp.float32)
    return result.astype(jnp.bfloat16)


def reference(latent, ln_gain, ln_bias, w_qkv, w_out, w_up, w_down):
    space_fn = partial(seq_block, layer_idx=0, ln_gain=ln_gain, ln_bias=ln_bias, w_qkv=w_qkv, w_out=w_out, w_up=w_up, w_down=w_down)
    spatial = lax.map(space_fn, latent[0])
    time_fn = partial(seq_block, layer_idx=1, ln_gain=ln_gain, ln_bias=ln_bias, w_qkv=w_qkv, w_out=w_out, w_up=w_up, w_down=w_down)
    temporal = lax.map(time_fn, jnp.swapaxes(spatial, 0, 1))
    return jnp.swapaxes(temporal, 0, 1)[None]
```

```python
import functools

import jax
import jax.numpy as jnp
from jax import lax
from jax.experimental import pallas as pl
from jax.experimental.pallas import tpu as pltpu
from jax.sharding import PartitionSpec as P

BF, F32 = jnp.bfloat16, jnp.float32
LN_EPS = 1e-6
LOG2E = 1.4426950408889634
LANES = 128
WIN = 2 * LANES
GROUP = 8
MESH = pl.DeviceIdType.MESH
VMEM_LIMIT = 66_000_000


def layer_norm(x, gain, bias):
    mean = jnp.mean(x, axis=-1, keepdims=True)
    c = x - mean
    var = jnp.mean(c * c, axis=-1, keepdims=True)
    return (c * lax.rsqrt(var + LN_EPS) * gain + bias).astype(BF)


def gelu(x):
    return 0.5 * x * (1.0 + jnp.tanh(0.7978845608028654 * (x + 0.044715 * (x * x * x))))


def dot(a, b):
    return jnp.dot(a, b, preferred_element_type=F32)


def dot_nt(a, b):
    return lax.dot_general(a, b, (((1,), (1,)), ((), ())), preferred_element_type=F32)


def softmax_rows(s, scale):
    m = jnp.max(s, axis=-1, keepdims=True)
    e = jnp.exp2((s - m) * (scale * LOG2E))
    return (e * (1.0 / jnp.sum(e, axis=-1, keepdims=True))).astype(BF)


def head_masks(j, hd):
    lane = lax.broadcasted_iota(jnp.int32, (1, WIN), 1)
    lo = j * (2 * hd - LANES)
    return [jnp.where((lane >= lo + i * hd) & (lane < lo + (i + 1) * hd), 1.0, 0.0).astype(BF) for i in range(2)]


def params(gain_ref, bias_ref, row):
    return gain_ref[row:row + 1, :].astype(F32), bias_ref[row:row + 1, :].astype(F32)


def greet(axis, n):
    me = lax.axis_index(axis)
    barrier = pltpu.get_barrier_semaphore()
    for r in range(1, n):
        pl.semaphore_signal(barrier, inc=1, device_id={axis: lax.rem(me + r, n)}, device_id_type=MESH)
    pl.semaphore_wait(barrier, n - 1)


def weight_copies(layer, srcs, dsts, sems):
    return [pltpu.make_async_copy(s.at[layer], d, sems.at[i]) for i, (s, d) in enumerate(zip(srcs, dsts))]


def spatial_kernel(hd, n, axis, x_ref, gain_ref, bias_ref, wqkv_h, wout_h, wup_h, wdown_h, recv_ref,
                   wqkv, wout, wup, wdown, a_ref, qkv_ref, o_ref, h_ref, hid_ref, y_ref,
                   w_sem, send_sem, recv_sem, own_sem):
    frames = pl.num_programs(0)
    step = pl.program_id(0)
    _, T, C = x_ref.shape
    share = T // n
    scale = hd ** -0.5
    me = lax.axis_index(axis)
    slot = lax.rem(step, 2)
    cps = weight_copies(0, (wqkv_h, wout_h, wup_h, wdown_h), (wqkv, wout, wup, wdown), w_sem)

    def send(r, sl, frame):
        peer = lax.rem(me + r, n)
        return pltpu.make_async_remote_copy(
            src_ref=y_ref.at[sl, pl.ds(pl.multiple_of(peer * share, share), share)],
            dst_ref=recv_ref.at[me * frames + frame],
            send_sem=send_sem.at[sl, r], recv_sem=recv_sem.at[r],
            device_id={axis: peer}, device_id_type=MESH)

    def keep(sl, frame):
        return pltpu.make_async_copy(y_ref.at[sl, pl.ds(pl.multiple_of(me * share, share), share)],
                                     recv_ref.at[me * frames + frame], own_sem.at[sl])

    @pl.when(step == 0)
    def _():
        for c in cps:
            c.start()

    a_ref[...] = layer_norm(x_ref[0].astype(F32), *params(gain_ref, bias_ref, 0))

    @pl.when(step == 0)
    def _():
        greet(axis, n)
        cps[0].wait()

    qkv_ref[...] = dot(a_ref[...], wqkv[...]).astype(BF)
    o_ref[:, 0:LANES] = jnp.zeros((T, LANES), BF)
    for j in range(C // (2 * hd)):
        c0 = j * LANES
        q, k, v = (qkv_ref[:, pl.ds(i * C + c0, WIN)] for i in range(3))
        o = sum(dot(softmax_rows(dot_nt(q, k * m), scale), v * m) for m in head_masks(j, hd)).astype(BF)
        o_ref[:, pl.ds(c0, LANES)] = o_ref[:, pl.ds(c0, LANES)] + o[:, :LANES]
        o_ref[:, pl.ds(c0 + LANES, LANES)] = o[:, LANES:]

    @pl.when(step == 0)
    def _():
        for c in cps[1:]:
            c.wait()

    @pl.when(step >= 2)
    def _():
        for r in range(1, n):
            send(r, slot, step - 2).wait_send()
        keep(slot, step - 2).wait()

    h = (x_ref[0].astype(F32) + dot(o_ref[...], wout[...])).astype(BF)
    h_ref[...] = h
    a_ref[...] = layer_norm(h.astype(F32), *params(gain_ref, bias_ref, 1))
    hid_ref[...] = gelu(dot(a_ref[...], wup[...])).astype(BF)
    y_ref[slot] = (h_ref[...].astype(F32) + dot(hid_ref[...], wdown[...])).astype(BF)
    for r in range(1, n):
        send(r, slot, step).start()
    keep(slot, step).start()

    @pl.when(step == frames - 1)
    def _():
        for sl, frame in ((1 - slot, step - 1), (slot, step)):
            for r in range(1, n):
                send(r, sl, frame).wait_send()
            keep(sl, frame).wait()
        for r in range(1, n):
            src = lax.rem(me + n - r, n)
            block = recv_ref.at[pl.ds(src * frames, frames)]
            pltpu.make_async_remote_copy(src_ref=block, dst_ref=block, send_sem=send_sem.at[0, r],
                                         recv_sem=recv_sem.at[r], device_id={axis: src},
                                         device_id_type=MESH).wait_recv()


def get_rows(ref, part, d):
    return jnp.concatenate([ref[part, i, d, :] for i in range(ref.shape[1])], axis=1)


def put_rows(ref, part, d, val):
    for i in range(ref.shape[1]):
        ref[part, i, d, :] = val[:, i * LANES:(i + 1) * LANES]


def temporal_kernel(hd, n, axis, x_ref, gain_ref, bias_ref, wqkv_h, wout_h, wup_h, wdown_h, out_ref,
                    wqkv, wout, wup, wdown, xs_ref, a_ref, qkv_ref, o_ref, h_ref, hid_ref, y_ref,
                    w_sem, send_sem, recv_sem, own_sem):
    steps = pl.num_programs(0)
    step = pl.program_id(0)
    F, G, C = x_ref.shape
    mine = F // n
    half = F // 2
    rows = half * G
    scale = hd ** -0.5
    me = lax.axis_index(axis)
    per = n // 2
    base = lax.div(me, per)
    cps = weight_copies(1, (wqkv_h, wout_h, wup_h, wdown_h), (wqkv, wout, wup, wdown), w_sem)

    def place(ref, who, st):
        return ref.at[:, pl.ds(pl.multiple_of(who * (steps * G) + st * G, G), G), :]

    def send(part, r, st):
        inner = lax.rem(me + r, per)
        peer = (1 - base if part == 0 else base) * per + inner
        return pltpu.make_async_remote_copy(
            src_ref=y_ref.at[part, pl.ds(inner * mine, mine)], dst_ref=place(out_ref, me, st),
            send_sem=send_sem.at[part, r], recv_sem=recv_sem.at[part, r],
            device_id={axis: peer}, device_id_type=MESH)

    def sends(part, st):
        return [send(part, r, st) for r in range(part, per)]

    def keep(st):
        return pltpu.make_async_copy(y_ref.at[1, pl.ds(lax.rem(me, per) * mine, mine)], place(out_ref, me, st),
                                     own_sem.at[0])

    @pl.when(step == 0)
    def _():
        for c in cps:
            c.start()

    for part in range(2):
        put_rows(xs_ref, part, pl.ds(0, rows), x_ref[pl.ds(part * half, half)].astype(F32).reshape(rows, C))
    for p in range(G):
        for part in range(2):
            a_ref[pl.ds(p * F + part * half, half), :] = layer_norm(
                get_rows(xs_ref, part, pl.ds(p, half, stride=G)), *params(gain_ref, bias_ref, 2))

    @pl.when(step == 0)
    def _():
        greet(axis, n)
        cps[0].wait()

    def project(i, _):
        r = pl.ds(pl.multiple_of(i * rows, rows), rows)
        qkv_ref[r, :] = dot(a_ref[r, :], wqkv[...]).astype(BF)
        return 0

    lax.fori_loop(0, 2, project, 0)

    o_ref[:, :, 0:LANES] = jnp.zeros((G, F, LANES), BF)
    for j in range(C // (2 * hd)):
        c0 = j * LANES
        m0, m1 = head_masks(j, hd)
        for p in range(G):
            q, k, v = (qkv_ref[pl.ds(p * F, F), pl.ds(i * C + c0, WIN)] for i in range(3))
            s = dot_nt(q, jnp.concatenate([k * m0, k * m1], axis=0))
            pr = jnp.concatenate([softmax_rows(s[:, :F], scale), softmax_rows(s[:, F:], scale)], axis=1)
            o = dot(pr, jnp.concatenate([v * m0, v * m1], axis=0)).astype(BF)
            o_ref[p, :, pl.ds(c0, LANES)] = o_ref[p, :, pl.ds(c0, LANES)] + o[:, :LANES]
            o_ref[p, :, pl.ds(c0 + LANES, LANES)] = o[:, LANES:]

    @pl.when(step == 0)
    def _():
        for c in cps[1:]:
            c.wait()

    for part in range(2):
        sel = 1 - base if part == 0 else base

        @pl.when(step >= 1)
        def _():
            for c in sends(part, step - 1):
                c.wait_send()
            if part == 1:
                keep(step - 1).wait()

        o = o_ref[:, pl.ds(pl.multiple_of(sel * half, half), half), :].reshape(rows, C)
        x = jnp.concatenate([get_rows(xs_ref, sel, pl.ds(p, half, stride=G)) for p in range(G)], axis=0)
        h = (x + dot(o, wout[...])).astype(BF)
        h_ref[...] = h
        a_ref[pl.ds(0, rows), :] = layer_norm(h.astype(F32), *params(gain_ref, bias_ref, 3))
        hid_ref[...] = gelu(dot(a_ref[pl.ds(0, rows), :], wup[...])).astype(BF)
        y = h_ref[...].astype(F32) + dot(hid_ref[...], wdown[...])
        for p in range(G):
            put_rows(xs_ref, sel, pl.ds(p, half, stride=G), y[p * half:(p + 1) * half])
        y_ref[part] = get_rows(xs_ref, sel, pl.ds(0, rows)).reshape(half, G, C).astype(BF)
        for c in sends(part, step):
            c.start()
        if part == 1:
            keep(step).start()

    @pl.when(step == steps - 1)
    def _():
        for part in range(2):
            for c in sends(part, step):
                c.wait_send()
        keep(step).wait()
        for part in range(2):
            for r in range(part, per):
                src = (1 - base if part == 0 else base) * per + lax.rem(me + per - r, per)
                block = out_ref.at[:, pl.ds(pl.multiple_of(src * (steps * G), steps * G), steps * G), :]
                pltpu.make_async_remote_copy(src_ref=block, dst_ref=block, send_sem=send_sem.at[part, r],
                                             recv_sem=recv_sem.at[part, r], device_id={axis: src},
                                             device_id_type=MESH).wait_recv()


def compiler_params(cid):
    return pltpu.CompilerParams(vmem_limit_bytes=VMEM_LIMIT, dimension_semantics=("arbitrary",), collective_id=cid,
                                has_side_effects=True)


def weight_scratch(C, H):
    return [pltpu.VMEM((C, 3 * C), BF), pltpu.VMEM((C, C), BF), pltpu.VMEM((C, H), BF), pltpu.VMEM((H, C), BF)]


def spatial_block(x, small, weights, hd, n, axis):
    frames, T, C = x.shape
    H = weights[2].shape[-1]
    any_spec = pl.BlockSpec(memory_space=pl.ANY)
    dma = pltpu.SemaphoreType.DMA
    return pl.pallas_call(
        functools.partial(spatial_kernel, hd, n, axis),
        grid=(frames,),
        in_specs=[pl.BlockSpec((1, T, C), lambda i: (i, 0, 0))]
        + [pl.BlockSpec(s.shape, lambda i: (0, 0)) for s in small] + [any_spec] * 4,
        out_specs=any_spec,
        out_shape=jax.ShapeDtypeStruct((n * frames, T // n, C), BF),
        scratch_shapes=weight_scratch(C, H) + [
            pltpu.VMEM((T, C), BF), pltpu.VMEM((T, 3 * C), BF), pltpu.VMEM((T, C), BF), pltpu.VMEM((T, C), BF),
            pltpu.VMEM((T, H), BF), pltpu.VMEM((2, T, C), BF),
            dma((4,)), dma((2, n)), dma((n,)), dma((2,))],
        compiler_params=compiler_params(0),
        name='spatial',
    )(x, *small, *weights)


def temporal_block(x, small, weights, hd, n, axis):
    F, share, C = x.shape
    H = weights[2].shape[-1]
    any_spec = pl.BlockSpec(memory_space=pl.ANY)
    dma = pltpu.SemaphoreType.DMA
    rows = F * GROUP // 2
    return pl.pallas_call(
        functools.partial(temporal_kernel, hd, n, axis),
        grid=(share // GROUP,),
        in_specs=[pl.BlockSpec((F, GROUP, C), lambda i: (0, i, 0))]
        + [pl.BlockSpec(s.shape, lambda i: (0, 0)) for s in small] + [any_spec] * 4,
        out_specs=any_spec,
        out_shape=jax.ShapeDtypeStruct((F // n, share * n, C), BF),
        scratch_shapes=weight_scratch(C, H) + [
            pltpu.VMEM((2, C // LANES, rows, LANES), F32), pltpu.VMEM((2 * rows, C), BF), pltpu.VMEM((2 * rows, 3 * C), BF),
            pltpu.VMEM((GROUP, F, C), BF), pltpu.VMEM((rows, C), BF),
            pltpu.VMEM((rows, H), BF), pltpu.VMEM((2, F // 2, GROUP, C), BF),
            dma((4,)), dma((2, n)), dma((2, n)), dma((1,))],
        compiler_params=compiler_params(1),
        name='temporal',
    )(x, *small, *weights)


def solution(mesh):
    n = mesh.shape['sp']
    act = P('data', 'sp', None, None)

    def local_run(latent, ln_gain, ln_bias, w_qkv, w_out, w_up, w_down):
        L, C, _, heads, hd = w_qkv.shape
        weights = (w_qkv.reshape(L, C, 3 * heads * hd), w_out.reshape(L, heads * hd, C), w_up, w_down)
        small = (ln_gain, ln_bias)
        mixed = spatial_block(latent[0], small, weights, hd, n, 'sp')
        return temporal_block(mixed, small, weights, hd, n, 'sp')[None]

    return jax.shard_map(local_run, mesh=mesh, in_specs=(act, P(), P(), P(), P(), P(), P()), out_specs=act, check_vma=False)
```

```python
import functools

import jax
import jax.numpy as jnp
from jax import lax
from jax.experimental import pallas as pl
from jax.experimental.pallas import tpu as pltpu
from jax.sharding import PartitionSpec as P

BF, F32 = jnp.bfloat16, jnp.float32
LN_EPS = 1e-6
LOG2E = 1.4426950408889634
LANES = 128
WIN = 2 * LANES
GROUP = 8
MESH = pl.DeviceIdType.MESH
VMEM_LIMIT = 66_000_000


def layer_norm(x, gain, bias):
    mean = jnp.mean(x, axis=-1, keepdims=True)
    c = x - mean
    var = jnp.mean(c * c, axis=-1, keepdims=True)
    return (c * lax.rsqrt(var + LN_EPS) * gain + bias).astype(BF)


def gelu(x):
    return 0.5 * x * (1.0 + jnp.tanh(0.7978845608028654 * (x + 0.044715 * (x * x * x))))


def dot(a, b):
    return jnp.dot(a, b, preferred_element_type=F32)


def dot_nt(a, b):
    return lax.dot_general(a, b, (((1,), (1,)), ((), ())), preferred_element_type=F32)


def softmax_rows(s, scale):
    m = jnp.max(s, axis=-1, keepdims=True)
    e = jnp.exp2((s - m) * (scale * LOG2E))
    return (e * (1.0 / jnp.sum(e, axis=-1, keepdims=True))).astype(BF)


def exp_rows(s, scale):
    return jnp.exp2((s - jnp.max(s, axis=-1, keepdims=True)) * (scale * LOG2E)).astype(BF)


def head_masks(j, hd):
    lane = lax.broadcasted_iota(jnp.int32, (1, WIN), 1)
    lo = j * (2 * hd - LANES)
    return [jnp.where((lane >= lo + i * hd) & (lane < lo + (i + 1) * hd), 1.0, 0.0).astype(BF) for i in range(2)]


def params(gain_ref, bias_ref, row):
    return gain_ref[row:row + 1, :].astype(F32), bias_ref[row:row + 1, :].astype(F32)


def greet(axis, n):
    me = lax.axis_index(axis)
    barrier = pltpu.get_barrier_semaphore()
    for r in range(1, n):
        pl.semaphore_signal(barrier, inc=1, device_id={axis: lax.rem(me + r, n)}, device_id_type=MESH)
    pl.semaphore_wait(barrier, n - 1)


def weight_copies(layer, srcs, dsts, sems):
    return [pltpu.make_async_copy(s.at[layer], d, sems.at[i]) for i, (s, d) in enumerate(zip(srcs, dsts))]


def spatial_kernel(hd, n, axis, x_ref, gain_ref, bias_ref, wqkv_h, wout_h, wup_h, wdown_h, recv_ref,
                   wqkv, wout, wup, wdown, a_ref, qkv_ref, o_ref, h_ref, hid_ref, y_ref,
                   w_sem, send_sem, recv_sem, own_sem):
    frames = pl.num_programs(0)
    step = pl.program_id(0)
    _, T, C = x_ref.shape
    share = T // n
    scale = hd ** -0.5
    me = lax.axis_index(axis)
    slot = lax.rem(step, 2)
    cps = weight_copies(0, (wqkv_h, wout_h, wup_h, wdown_h), (wqkv, wout, wup, wdown), w_sem)

    def send(r, sl, frame):
        peer = lax.rem(me + r, n)
        return pltpu.make_async_remote_copy(
            src_ref=y_ref.at[sl, pl.ds(pl.multiple_of(peer * share, share), share)],
            dst_ref=recv_ref.at[me * frames + frame],
            send_sem=send_sem.at[sl, r], recv_sem=recv_sem.at[r],
            device_id={axis: peer}, device_id_type=MESH)

    def keep(sl, frame):
        return pltpu.make_async_copy(y_ref.at[sl, pl.ds(pl.multiple_of(me * share, share), share)],
                                     recv_ref.at[me * frames + frame], own_sem.at[sl])

    @pl.when(step == 0)
    def _():
        for c in cps:
            c.start()

    a_ref[...] = layer_norm(x_ref[0].astype(F32), *params(gain_ref, bias_ref, 0))

    @pl.when(step == 0)
    def _():
        greet(axis, n)
        cps[0].wait()

    qkv_ref[...] = dot(a_ref[...], wqkv[...]).astype(BF)
    o_ref[:, 0:LANES] = jnp.zeros((T, LANES), BF)
    for j in range(C // (2 * hd)):
        c0 = j * LANES
        q, k, v = (qkv_ref[:, pl.ds(i * C + c0, WIN)] for i in range(3))
        o = sum(dot(softmax_rows(dot_nt(q, k * m), scale), v * m) for m in head_masks(j, hd)).astype(BF)
        o_ref[:, pl.ds(c0, LANES)] = o_ref[:, pl.ds(c0, LANES)] + o[:, :LANES]
        o_ref[:, pl.ds(c0 + LANES, LANES)] = o[:, LANES:]

    @pl.when(step == 0)
    def _():
        for c in cps[1:]:
            c.wait()

    @pl.when(step >= 2)
    def _():
        for r in range(1, n):
            send(r, slot, step - 2).wait_send()
        keep(slot, step - 2).wait()

    h = (x_ref[0].astype(F32) + dot(o_ref[...], wout[...])).astype(BF)
    h_ref[...] = h
    a_ref[...] = layer_norm(h.astype(F32), *params(gain_ref, bias_ref, 1))
    hid_ref[...] = gelu(dot(a_ref[...], wup[...])).astype(BF)
    y_ref[slot] = (h_ref[...].astype(F32) + dot(hid_ref[...], wdown[...])).astype(BF)
    for r in range(1, n):
        send(r, slot, step).start()
    keep(slot, step).start()

    @pl.when(step == frames - 1)
    def _():
        for sl, frame in ((1 - slot, step - 1), (slot, step)):
            for r in range(1, n):
                send(r, sl, frame).wait_send()
            keep(sl, frame).wait()
        for r in range(1, n):
            src = lax.rem(me + n - r, n)
            block = recv_ref.at[pl.ds(src * frames, frames)]
            pltpu.make_async_remote_copy(src_ref=block, dst_ref=block, send_sem=send_sem.at[0, r],
                                         recv_sem=recv_sem.at[r], device_id={axis: src},
                                         device_id_type=MESH).wait_recv()


def get_rows(ref, part, d):
    return jnp.concatenate([ref[part, i, d, :] for i in range(ref.shape[1])], axis=1)


def put_rows(ref, part, d, val):
    for i in range(ref.shape[1]):
        ref[part, i, d, :] = val[:, i * LANES:(i + 1) * LANES]


def temporal_kernel(hd, n, axis, x_ref, gain_ref, bias_ref, wqkv_h, wout_h, wup_h, wdown_h, out_ref,
                    wqkv, wout, wup, wdown, xs_ref, a_ref, qkv_ref, o_ref, h_ref, hid_ref, y_ref,
                    w_sem, send_sem, recv_sem, own_sem):
    steps = pl.num_programs(0)
    step = pl.program_id(0)
    F, G, C = x_ref.shape
    mine = F // n
    half = F // 2
    rows = half * G
    scale = hd ** -0.5
    me = lax.axis_index(axis)
    per = n // 2
    base = lax.div(me, per)
    cps = weight_copies(1, (wqkv_h, wout_h, wup_h, wdown_h), (wqkv, wout, wup, wdown), w_sem)

    def place(ref, who, st):
        return ref.at[:, pl.ds(pl.multiple_of(who * (steps * G) + st * G, G), G), :]

    def send(part, r, st):
        inner = lax.rem(me + r, per)
        peer = (1 - base if part == 0 else base) * per + inner
        return pltpu.make_async_remote_copy(
            src_ref=y_ref.at[part, pl.ds(inner * mine, mine)], dst_ref=place(out_ref, me, st),
            send_sem=send_sem.at[part, r], recv_sem=recv_sem.at[part, r],
            device_id={axis: peer}, device_id_type=MESH)

    def sends(part, st):
        return [send(part, r, st) for r in range(part, per)]

    def keep(st):
        return pltpu.make_async_copy(y_ref.at[1, pl.ds(lax.rem(me, per) * mine, mine)], place(out_ref, me, st),
                                     own_sem.at[0])

    @pl.when(step == 0)
    def _():
        for c in cps:
            c.start()

    for part in range(2):
        put_rows(xs_ref, part, pl.ds(0, rows), x_ref[pl.ds(part * half, half)].astype(F32).reshape(rows, C))
    for p in range(G):
        for part in range(2):
            a_ref[pl.ds(p * F + part * half, half), :] = layer_norm(
                get_rows(xs_ref, part, pl.ds(p, half, stride=G)), *params(gain_ref, bias_ref, 2))

    @pl.when(step == 0)
    def _():
        greet(axis, n)
        cps[0].wait()

    def project(i, _):
        r = pl.ds(pl.multiple_of(i * rows, rows), rows)
        qkv_ref[r, :] = dot(a_ref[r, :], wqkv[...]).astype(BF)
        return 0

    lax.fori_loop(0, 2, project, 0)

    o_ref[:, :, 0:LANES] = jnp.zeros((G, F, LANES), BF)

    def scores(j):
        m0, m1 = head_masks(j, hd)
        out = []
        for p in range(G):
            q, k = (qkv_ref[pl.ds(p * F, F), pl.ds(i * C + j * LANES, WIN)] for i in range(2))
            out.append(dot_nt(q, jnp.concatenate([k * m0, k * m1], axis=0)))
        return out

    def weigh(j, ss):
        c0 = j * LANES
        m0, m1 = head_masks(j, hd)
        tally = jnp.concatenate([jnp.broadcast_to(m0, (F, WIN)), jnp.broadcast_to(1 - m0, (F, WIN))], axis=0)
        es = [jnp.concatenate([exp_rows(s[:, :F], scale), exp_rows(s[:, F:], scale)], axis=1) for s in ss]
        nums, dens = [], []
        for p in range(G):
            v = qkv_ref[pl.ds(p * F, F), pl.ds(2 * C + c0, WIN)]
            nums.append(dot(es[p], jnp.concatenate([v * m0, v * m1], axis=0)))
            dens.append(dot(es[p], tally))
        for p in range(G):
            o = (nums[p] / dens[p]).astype(BF)
            o_ref[p, :, pl.ds(c0, LANES)] = o_ref[p, :, pl.ds(c0, LANES)] + o[:, :LANES]
            o_ref[p, :, pl.ds(c0 + LANES, LANES)] = o[:, LANES:]

    pairs = C // (2 * hd)
    held = scores(0)
    for j in range(pairs):
        following = scores(j + 1) if j + 1 < pairs else None
        weigh(j, held)
        held = following

    @pl.when(step == 0)
    def _():
        for c in cps[1:]:
            c.wait()

    for part in range(2):
        sel = 1 - base if part == 0 else base

        @pl.when(step >= 1)
        def _():
            for c in sends(part, step - 1):
                c.wait_send()
            if part == 1:
                keep(step - 1).wait()

        o = o_ref[:, pl.ds(pl.multiple_of(sel * half, half), half), :].reshape(rows, C)
        x = jnp.concatenate([get_rows(xs_ref, sel, pl.ds(p, half, stride=G)) for p in range(G)], axis=0)
        h = (x + dot(o, wout[...])).astype(BF)
        h_ref[...] = h
        a_ref[pl.ds(0, rows), :] = layer_norm(h.astype(F32), *params(gain_ref, bias_ref, 3))
        hid_ref[...] = gelu(dot(a_ref[pl.ds(0, rows), :], wup[...])).astype(BF)
        y = h_ref[...].astype(F32) + dot(hid_ref[...], wdown[...])
        for p in range(G):
            put_rows(xs_ref, sel, pl.ds(p, half, stride=G), y[p * half:(p + 1) * half])
        y_ref[part] = get_rows(xs_ref, sel, pl.ds(0, rows)).reshape(half, G, C).astype(BF)
        for c in sends(part, step):
            c.start()
        if part == 1:
            keep(step).start()

    @pl.when(step == steps - 1)
    def _():
        for part in range(2):
            for c in sends(part, step):
                c.wait_send()
        keep(step).wait()
        for part in range(2):
            for r in range(part, per):
                src = (1 - base if part == 0 else base) * per + lax.rem(me + per - r, per)
                block = out_ref.at[:, pl.ds(pl.multiple_of(src * (steps * G), steps * G), steps * G), :]
                pltpu.make_async_remote_copy(src_ref=block, dst_ref=block, send_sem=send_sem.at[part, r],
                                             recv_sem=recv_sem.at[part, r], device_id={axis: src},
                                             device_id_type=MESH).wait_recv()


def compiler_params(cid):
    return pltpu.CompilerParams(vmem_limit_bytes=VMEM_LIMIT, dimension_semantics=("arbitrary",), collective_id=cid,
                                has_side_effects=True)


def weight_scratch(C, H):
    return [pltpu.VMEM((C, 3 * C), BF), pltpu.VMEM((C, C), BF), pltpu.VMEM((C, H), BF), pltpu.VMEM((H, C), BF)]


def spatial_block(x, small, weights, hd, n, axis):
    frames, T, C = x.shape
    H = weights[2].shape[-1]
    any_spec = pl.BlockSpec(memory_space=pl.ANY)
    dma = pltpu.SemaphoreType.DMA
    return pl.pallas_call(
        functools.partial(spatial_kernel, hd, n, axis),
        grid=(frames,),
        in_specs=[pl.BlockSpec((1, T, C), lambda i: (i, 0, 0))]
        + [pl.BlockSpec(s.shape, lambda i: (0, 0)) for s in small] + [any_spec] * 4,
        out_specs=any_spec,
        out_shape=jax.ShapeDtypeStruct((n * frames, T // n, C), BF),
        scratch_shapes=weight_scratch(C, H) + [
            pltpu.VMEM((T, C), BF), pltpu.VMEM((T, 3 * C), BF), pltpu.VMEM((T, C), BF), pltpu.VMEM((T, C), BF),
            pltpu.VMEM((T, H), BF), pltpu.VMEM((2, T, C), BF),
            dma((4,)), dma((2, n)), dma((n,)), dma((2,))],
        compiler_params=compiler_params(0),
        name='spatial',
    )(x, *small, *weights)


def temporal_block(x, small, weights, hd, n, axis):
    F, share, C = x.shape
    H = weights[2].shape[-1]
    any_spec = pl.BlockSpec(memory_space=pl.ANY)
    dma = pltpu.SemaphoreType.DMA
    rows = F * GROUP // 2
    return pl.pallas_call(
        functools.partial(temporal_kernel, hd, n, axis),
        grid=(share // GROUP,),
        in_specs=[pl.BlockSpec((F, GROUP, C), lambda i: (0, i, 0))]
        + [pl.BlockSpec(s.shape, lambda i: (0, 0)) for s in small] + [any_spec] * 4,
        out_specs=any_spec,
        out_shape=jax.ShapeDtypeStruct((F // n, share * n, C), BF),
        scratch_shapes=weight_scratch(C, H) + [
            pltpu.VMEM((2, C // LANES, rows, LANES), F32), pltpu.VMEM((2 * rows, C), BF), pltpu.VMEM((2 * rows, 3 * C), BF),
            pltpu.VMEM((GROUP, F, C), BF), pltpu.VMEM((rows, C), BF),
            pltpu.VMEM((rows, H), BF), pltpu.VMEM((2, F // 2, GROUP, C), BF),
            dma((4,)), dma((2, n)), dma((2, n)), dma((1,))],
        compiler_params=compiler_params(1),
        name='temporal',
    )(x, *small, *weights)


def solution(mesh):
    n = mesh.shape['sp']
    act = P('data', 'sp', None, None)

    def local_run(latent, ln_gain, ln_bias, w_qkv, w_out, w_up, w_down):
        L, C, _, heads, hd = w_qkv.shape
        weights = (w_qkv.reshape(L, C, 3 * heads * hd), w_out.reshape(L, heads * hd, C), w_up, w_down)
        small = (ln_gain, ln_bias)
        mixed = spatial_block(latent[0], small, weights, hd, n, 'sp')
        return temporal_block(mixed, small, weights, hd, n, 'sp')[None]

    return jax.shard_map(local_run, mesh=mesh, in_specs=(act, P(), P(), P(), P(), P(), P()), out_specs=act, check_vma=False)
```
